32 devices in a mesh: row: 4 (over y, x), col: 8 (over z, core).
Axes of the slice: x: 2, y: 2, z: 4, core: 2. Of those that a mesh axis runs over, the one named last changes fastest.
Arguments:
- source_blocks: float32 [8192, 24576], P('row', 'col'), may hold values from -6 to 6
Outputs:
- target_blocks: float32 [4096, 49152], P('row', 'col')
- column_sums: float32 [49152], P('col')
- frobenius: float32 [], replicated
The draws below stay inside these ranges and needn't reach their ends.
All inputs are finite; a program needn't handle non-finite values.
Results may differ from the reference program's by a relative error of at most 0.00002.
Values sent between devices are 32-bit elements; how exact they have to be, the bound alone decides.
A program may use at most 192 MiB of HBM per device.

```python
import math
import jax
import jax.numpy as jnp
from jax import lax

N = 24576
SB = 128
RB = 2
TB = 512
M = 8192
E = 12
N_ROW = 4
N_COL = 8


def strengthened(drawn, own_key, source, target, parts, factor):
    owner, partner = [(jnp.arange(drawn.shape[dim]) // (drawn.shape[dim] // parts)).reshape([-1 if axis == dim else 1 for axis in range(drawn.ndim)]) for dim in (source, target)]
    chosen = jax.random.permutation(own_key, parts)[partner]
    strong = (owner == chosen) | (owner == (partner + parts // 2) % parts)
    return jnp.where(strong, factor * drawn, drawn)


def block_scale(key, shape, cuts, smallest, top_value):
    factor_of, own = 1.0, jax.random.fold_in(key, 6)
    for dim, blocks in cuts:
        steps = jnp.exp(jax.random.uniform(jax.random.fold_in(own, dim), (blocks,), jnp.float32, smallest / len(cuts), top_value / len(cuts)))
        factor_of = factor_of * jnp.repeat(steps, shape[dim] // blocks).reshape([-1 if axis == dim else 1 for axis in range(len(shape))])
    return factor_of


def noise_with(own_key, shape, width, bound, split, heavy, held_as=jnp.bfloat16):
    array = width * jax.random.normal(own_key, shape, jnp.float32)
    if split:
        array = array * block_scale(own_key, shape, split, -0.22, 0.18)
    return jnp.clip(strengthened(array, jax.random.fold_in(own_key, 3), *heavy), -bound, bound).astype(held_as)


def setup_inputs(seed: int = 0) -> dict:
    splits = jax.random.split(jax.random.key(seed), 2)
    return {
        "source_blocks": noise_with(splits[0], (M, N), 1.0, 6.0, ((0, 4), (1, 8)), (0, 1, 8, 2.0), jnp.float32),
    }


def reference(source_blocks):
    row_count = N_ROW
    col_count = N_COL
    cells = source_blocks.reshape(row_count, M // row_count // SB, SB, col_count, N // col_count // SB, SB)
    matrix = cells.transpose(1, 0, 2, 4, 3, 5).reshape(M, N)
    pieces = matrix.reshape(RB, 2, 4, row_count // 4, TB, E, 2, col_count // 4, TB)
    target_blocks = pieces.transpose(3, 2, 0, 4, 7, 1, 6, 5, 8).reshape(M // 2, 2 * N)
    scale = 1.0 / math.sqrt(M)
    totals = lax.optimization_barrier(jnp.sum(matrix, axis=0)) * scale
    grouped = totals.reshape(E, 2, col_count // 4, TB).transpose(2, 1, 0, 3)
    column_sums = jnp.broadcast_to(grouped[:, None], (col_count // 4, 2, 2, E, TB)).reshape(2 * N)
    frobenius = jnp.sqrt(jnp.sum(matrix * matrix) / (M * N))
    return (target_blocks, column_sums, frobenius)
```

```python
import functools
import math

import jax
import jax.numpy as jnp
from jax import lax
from jax.experimental import pallas as pl
from jax.experimental.pallas import tpu as pltpu
from jax.sharding import PartitionSpec as P

SB = 128
SUB = 8
ORDER = (15, 5, 10, 11, 3, 7, 14, 1, 9, 13, 2, 6, 8, 12, 4)


def flipped(index, bits):
    low = (index % 2 + bits % 2) % 2
    high = (index // 2 + bits // 2) % 2
    return high * 2 + low


def redistribute(groups, count, scale, x, out, cols, fro, own, ring, acc, part, slots, gsq, gslots,
                 send, recv, psend, precv, gsend, grecv, osem, rsem):
    row_groups, col_groups = groups
    deep, _, _, tiles, wide = x.shape[:5]
    me_row, me_col = lax.axis_index("row"), lax.axis_index("col")
    r, g = me_row % 4, me_row // 4
    c, h = me_col % 4, me_col // 4
    me = r * 4 + c

    peers = []
    for bits in ORDER:
        tr, tc = flipped(r, bits % 4), flipped(c, bits // 4)
        peers.append((bits, tr, tc, {"row": g * 4 + tr, "col": h * 4 + tc}))
    others = []
    for dg in range(row_groups):
        for dh in range(col_groups):
            if dg or dh:
                og, oh = (g + dg) % row_groups, (h + dh) % col_groups
                others.append((dg * col_groups + dh, {"row": og * 4 + r, "col": oh * 4 + c}))

    barrier = pltpu.get_barrier_semaphore()
    for _, _, _, device in peers:
        pl.semaphore_signal(barrier, inc=1, device_id=device)
    for _, device in others:
        pl.semaphore_signal(barrier, inc=1, device_id=device)
    pl.semaphore_wait(barrier, len(peers) + len(others))

    copies = []
    for s in range(deep):
        for bits, tr, tc, device in peers:
            copy = pltpu.make_async_remote_copy(
                src_ref=x.at[s, tc // 2, tr, :, :, tc % 2],
                dst_ref=out.at[s, r, :, :, c],
                send_sem=send.at[bits, s],
                recv_sem=recv.at[bits, s],
                device_id=device,
            )
            copy.start()
            copies.append(copy)

    own_in = [pltpu.make_async_copy(x.at[s, c // 2, r, :, :, c % 2], own.at[s], osem.at[s])
              for s in range(deep)]
    own_out = [pltpu.make_async_copy(own.at[s], out.at[s, r, :, :, c], osem.at[s])
               for s in range(deep)]
    for copy in own_in:
        copy.start()

    blocks = deep * 8

    def load(b):
        return pltpu.make_async_copy(x.at[b // 8, b // 4 % 2, b % 4], ring.at[b % 2], rsem.at[b % 2])

    load(0).start()
    load(1).start()
    acc[...] = jnp.zeros_like(acc)
    for i in range(deep):
        own_in[i].wait()
        own_out[i].start()

    def block(b, sq):
        load(b).wait()

        def column(e, sq):
            v = ring[b % 2, :, e]
            acc[e] += jnp.sum(v, axis=0)
            return sq + jnp.sum(v * v, axis=(0, 1))

        sq = lax.fori_loop(0, wide, column, sq)

        @pl.when(b + 2 < blocks)
        def _():
            load(b + 2).start()

        return sq

    sq = lax.fori_loop(0, blocks, block, jnp.zeros((SUB, SB), jnp.float32))
    part[...] = jnp.zeros_like(part)
    for k in range(2):
        for e in range(wide):
            part[k, e:e + 1, :] = jnp.sum(acc[e, k], axis=0, keepdims=True)
        part[k, wide:wide + 1, :] = jnp.sum(sq, axis=0, keepdims=True)
    for copy in own_out:
        copy.wait()

    small = []
    for bits, tr, tc, device in peers:
        copy = pltpu.make_async_remote_copy(
            src_ref=part.at[tc % 2], dst_ref=slots.at[me],
            send_sem=psend.at[bits], recv_sem=precv.at[bits], device_id=device,
        )
        copy.start()
        small.append(copy)
    slots[me] = part[c % 2]
    for copy in small:
        copy.wait()

    total = slots[0, wide:wide + 1, :]
    for i in range(1, 16):
        total += slots[i, wide:wide + 1, :]
    gsq[...] = jnp.broadcast_to(total, gsq.shape)
    for q in range(4):
        s = slots[q, :wide, :]
        for p in range(1, 4):
            s += slots[p * 4 + q, :wide, :]
        cols[pl.ds(q, wide, stride=4), :] = s * scale

    tail = []
    for i, device in others:
        copy = pltpu.make_async_remote_copy(
            src_ref=gsq, dst_ref=gslots.at[g * col_groups + h],
            send_sem=gsend.at[i], recv_sem=grecv.at[i], device_id=device,
        )
        copy.start()
        tail.append(copy)
    gslots[g * col_groups + h] = gsq[...]
    for copy in tail:
        copy.wait()
    total = gslots[0]
    for i in range(1, row_groups * col_groups):
        total += gslots[i]
    fro[0, 0] = jnp.sqrt(jnp.broadcast_to(jnp.sum(total[0:1, :]) / count, (1, SB)))[0, 0]

    for copy in copies:
        copy.wait()


def per_device(source_blocks):
    local_rows, local_cols = source_blocks.shape
    row_count, col_count = lax.axis_size("row"), lax.axis_size("col")
    groups = (row_count // 4, col_count // 4)
    total_rows = local_rows * row_count
    count = total_rows * local_cols * col_count
    deep, wide, tiles = local_rows // (8 * SB), local_cols // (2 * SB), SB // SUB
    x = source_blocks.reshape(local_rows // SUB, SUB, local_cols // SB, SB).transpose(0, 2, 1, 3)
    x = x.reshape(deep, 2, 4, tiles, wide, 2, SUB, SB)
    f32 = jnp.float32
    rows = -(-(wide + 1) // SUB) * SUB
    n = groups[0] * groups[1]
    dma = pltpu.SemaphoreType.DMA
    out, cols, fro = pl.pallas_call(
        functools.partial(redistribute, groups, float(count), 1.0 / math.sqrt(total_rows)),
        out_shape=(
            jax.ShapeDtypeStruct((deep, 4, tiles, wide, 4, SUB, SB), f32),
            jax.ShapeDtypeStruct((wide * 4, SB), f32),
            jax.ShapeDtypeStruct((1, 1), f32),
        ),
        in_specs=[pl.BlockSpec(memory_space=pl.ANY)],
        out_specs=(
            pl.BlockSpec(memory_space=pl.ANY),
            pl.BlockSpec(memory_space=pltpu.VMEM),
            pl.BlockSpec(memory_space=pltpu.SMEM),
        ),
        scratch_shapes=[
            pltpu.VMEM((deep, tiles, wide, SUB, SB), f32),
            pltpu.VMEM((2, tiles, wide, 2, SUB, SB), f32),
            pltpu.VMEM((wide, 2, SUB, SB), f32),
            pltpu.VMEM((2, rows, SB), f32),
            pltpu.VMEM((16, rows, SB), f32),
            pltpu.VMEM((SUB, SB), f32),
            pltpu.VMEM((n, SUB, SB), f32),
            dma((16, deep)), dma((16, deep)), dma((16,)), dma((16,)),
            dma((n,)), dma((n,)), dma((deep,)), dma((2,)),
        ],
        compiler_params=pltpu.CompilerParams(
            collective_id=0, has_side_effects=True, vmem_limit_bytes=16 * 2**20
        ),
        name="redistribute",
    )(x)
    target = out.reshape(deep * 4 * tiles, wide * 4, SUB, SB).transpose(0, 2, 1, 3)
    target = target.reshape(deep * 4 * SB, wide * 4 * SB)
    return target, cols.reshape(wide * 4 * SB), fro.reshape(())


def solution(mesh):
    return jax.shard_map(
        per_device,
        mesh=mesh,
        in_specs=(P("row", "col"),),
        out_specs=(P("row", "col"), P("col"), P()),
        check_vma=False,
    )
```

```python
import functools
import math

import jax
import jax.numpy as jnp
from jax import lax
from jax.experimental import pallas as pl
from jax.experimental.pallas import tpu as pltpu
from jax.sharding import PartitionSpec as P

SB = 128
SUB = 8
QUEUES = ((15, 8, 11, 12, 9, 10, 13, 14), (7, 2, 3, 6), (5, 1), (4,))
FLIPS = (3, 1, 0, 0)
STARTS = ((3, 2, 1, 1), (3, 1, 1, 0))


def flipped(index, bits):
    low = (index % 2 + bits % 2) % 2
    high = (index // 2 + bits // 2) % 2
    return high * 2 + low


def redistribute(groups, count, scale, x, out, cols, fro, own, ring, acc, part, slots, gsq, gslots,
                 send, recv, psend, precv, gsend, grecv, osem, rsem):
    row_groups, col_groups = groups
    deep, _, _, tiles, wide = x.shape[:5]
    me_row, me_col = lax.axis_index("row"), lax.axis_index("col")
    r, g = me_row % 4, me_row // 4
    c, h = me_col % 4, me_col // 4
    me = r * 4 + c

    core = c % 2
    peers = []
    for bits in range(1, 16):
        tr, tc = flipped(r, bits % 4), flipped(c, bits // 4)
        peers.append((bits, tr, tc, {"row": g * 4 + tr, "col": h * 4 + tc}))
    others = []
    for dg in range(row_groups):
        for dh in range(col_groups):
            if dg or dh:
                og, oh = (g + dg) % row_groups, (h + dh) % col_groups
                others.append((dg * col_groups + dh, {"row": og * 4 + r, "col": oh * 4 + c}))

    barrier = pltpu.get_barrier_semaphore()
    for _, _, _, device in peers:
        pl.semaphore_signal(barrier, inc=1, device_id=device)
    for _, device in others:
        pl.semaphore_signal(barrier, inc=1, device_id=device)
    pl.semaphore_wait(barrier, len(peers) + len(others))

    queues, small, tail = [], [], []
    for queue, flip in zip(QUEUES, FLIPS):
        queues.append([])
        for s in range(deep):
            for first in queue:
                bits = first + ((first ^ flip) - first) * core
                tr, tc = flipped(r, bits % 4), flipped(c, bits // 4)
                queues[-1].append(pltpu.make_async_remote_copy(
                    src_ref=x.at[s, tc // 2, tr, :, :, tc % 2],
                    dst_ref=out.at[s, r, :, :, c],
                    send_sem=send.at[bits, s],
                    recv_sem=recv.at[bits, s],
                    device_id={"row": g * 4 + tr, "col": h * 4 + tc},
                ))
    copies = [copy for queue in queues for copy in queue]
    waiting = [list(queue) for queue in queues]

    def start(counts):
        for queue, count in zip(waiting, counts):
            for copy in queue[:count]:
                copy.start()
            del queue[:count]

    own_in = [pltpu.make_async_copy(x.at[s, c // 2, r, :, :, c % 2], own.at[s], osem.at[s])
              for s in range(deep)]
    own_out = [pltpu.make_async_copy(own.at[s], out.at[s, r, :, :, c], osem.at[s])
               for s in range(deep)]
    blocks = deep * 8

    def load(b):
        return pltpu.make_async_copy(x.at[b // 8, b // 4 % 2, b % 4], ring.at[b % 2], rsem.at[b % 2])

    def block(b, sq):
        load(b).wait()

        def column(e, sq):
            v = ring[b % 2, :, e]
            acc[e] += jnp.sum(v, axis=0)
            return sq + jnp.sum(v * v, axis=(0, 1))

        sq = lax.fori_loop(0, wide, column, sq)

        @pl.when(b + 2 < blocks)
        def _():
            load(b + 2).start()

        return sq

    def sums():
        load(0).start()
        load(1).start()
        for copy in own_in:
            copy.start()
        acc[...] = jnp.zeros_like(acc)
        sq = lax.fori_loop(0, blocks, block, jnp.zeros((SUB, SB), jnp.float32))
        part[...] = jnp.zeros_like(part)
        for k in range(2):
            for e in range(wide):
                part[k, e:e + 1, :] = jnp.sum(acc[e, k], axis=0, keepdims=True)
            part[k, wide:wide + 1, :] = jnp.sum(sq, axis=0, keepdims=True)
        for i in range(deep):
            own_in[i].wait()
            own_out[i].start()
        for bits, tr, tc, device in peers:
            copy = pltpu.make_async_remote_copy(
                src_ref=part.at[tc % 2], dst_ref=slots.at[me],
                send_sem=psend.at[bits], recv_sem=precv.at[bits], device_id=device,
            )
            copy.start()
            small.append(copy)
        slots[me] = part[c % 2]

    def fold():
        for copy in small:
            copy.wait()
        total = slots[0, wide:wide + 1, :]
        for i in range(1, 16):
            total += slots[i, wide:wide + 1, :]
        gsq[...] = jnp.broadcast_to(total, gsq.shape)
        for q in range(4):
            s = slots[q, :wide, :]
            for p in range(1, 4):
                s += slots[p * 4 + q, :wide, :]
            cols[pl.ds(q, wide, stride=4), :] = s * scale
        for i, device in others:
            copy = pltpu.make_async_remote_copy(
                src_ref=gsq, dst_ref=gslots.at[g * col_groups + h],
                send_sem=gsend.at[i], recv_sem=grecv.at[i], device_id=device,
            )
            copy.start()
            tail.append(copy)
        gslots[g * col_groups + h] = gsq[...]
        for copy in own_out:
            copy.wait()

    start(STARTS[0])
    sums()
    start(STARTS[1])
    fold()
    start([len(queue) for queue in waiting])
    for copy in tail:
        copy.wait()
    total = gslots[0]
    for i in range(1, row_groups * col_groups):
        total += gslots[i]
    fro[0, 0] = jnp.sqrt(jnp.broadcast_to(jnp.sum(total[0:1, :]) / count, (1, SB)))[0, 0]
    for copy in copies:
        copy.wait()


def settle(pieces, held, out, sem):
    copies = [pltpu.make_async_copy(held.at[i // 4, i % 4], out.at[i // 4, i % 4], sem.at[i])
              for i in range(pieces)]
    for copy in copies:
        copy.start()
    for copy in copies:
        copy.wait()


def per_device(source_blocks):
    local_rows, local_cols = source_blocks.shape
    row_count, col_count = lax.axis_size("row"), lax.axis_size("col")
    groups = (row_count // 4, col_count // 4)
    total_rows = local_rows * row_count
    count = total_rows * local_cols * col_count
    deep, wide, tiles = local_rows // (8 * SB), local_cols // (2 * SB), SB // SUB
    x = source_blocks.reshape(local_rows // SUB, SUB, local_cols // SB, SB).transpose(0, 2, 1, 3)
    x = x.reshape(deep, 2, 4, tiles, wide, 2, SUB, SB)
    f32 = jnp.float32
    rows = -(-(wide + 1) // SUB) * SUB
    n = groups[0] * groups[1]
    dma = pltpu.SemaphoreType.DMA
    out, cols, fro = pl.pallas_call(
        functools.partial(redistribute, groups, float(count), 1.0 / math.sqrt(total_rows)),
        out_shape=(
            jax.ShapeDtypeStruct((deep, 4, tiles, wide, 4, SUB, SB), f32),
            jax.ShapeDtypeStruct((wide * 4, SB), f32),
            jax.ShapeDtypeStruct((1, 1), f32),
        ),
        in_specs=[pl.BlockSpec(memory_space=pl.ANY)],
        out_specs=(
            pl.BlockSpec(memory_space=pl.ANY),
            pl.BlockSpec(memory_space=pltpu.VMEM),
            pl.BlockSpec(memory_space=pltpu.SMEM),
        ),
        scratch_shapes=[
            pltpu.VMEM((deep, tiles, wide, SUB, SB), f32),
            pltpu.VMEM((2, tiles, wide, 2, SUB, SB), f32),
            pltpu.VMEM((wide, 2, SUB, SB), f32),
            pltpu.VMEM((2, rows, SB), f32),
            pltpu.VMEM((16, rows, SB), f32),
            pltpu.VMEM((SUB, SB), f32),
            pltpu.VMEM((n, SUB, SB), f32),
            dma((16, deep)), dma((16, deep)), dma((16,)), dma((16,)),
            dma((n,)), dma((n,)), dma((deep,)), dma((2,)),
        ],
        compiler_params=pltpu.CompilerParams(
            collective_id=0, has_side_effects=True, vmem_limit_bytes=16 * 2**20
        ),
        name="redistribute",
    )(x)
    pieces = deep * 4
    out = pl.pallas_call(
        functools.partial(settle, pieces),
        out_shape=jax.ShapeDtypeStruct(out.shape, f32),
        in_specs=[pl.BlockSpec(memory_space=pl.ANY)],
        out_specs=pl.BlockSpec(memory_space=pl.ANY),
        scratch_shapes=[dma((pieces,))],
        compiler_params=pltpu.CompilerParams(vmem_limit_bytes=2**20),
        name="settle",
    )(out)
    target = out.reshape(deep * 4 * tiles, wide * 4, SUB, SB).transpose(0, 2, 1, 3)
    target = target.reshape(deep * 4 * SB, wide * 4 * SB)
    return target, cols.reshape(wide * 4 * SB), fro.reshape(())


def solution(mesh):
    return jax.shard_map(
        per_device,
        mesh=mesh,
        in_specs=(P("row", "col"),),
        out_specs=(P("row", "col"), P("col"), P()),
        check_vma=False,
    )
```
